32 devices in a mesh: gx: 8 (over y, x, core), gy: 4 (over z).
Axes of the slice: x: 2, y: 2, z: 4, core: 2. Of those that a mesh axis runs over, the one named last changes fastest.
Arguments:
- sky_interface_transfers: bfloat16 [4, 384, 1024], P(None, 'gy', 'gx'), may hold values from -6 to 6
- coupling_matrix_enlarged: bfloat16 [384, 1024, 128], P('gy', 'gx'), may hold values from -0.5 to 0.5
- piece_keeper_part: int32 [8, 384, 1], P('gx', 'gy'), may hold values from 0 to 31; in each aligned block of 96 rows (0 to 95, 96 to 191, ..., all dimensions but the last counted through in order) at most 6 rows name the same one
- receiving_part_line: int32 [8, 384], P('gx', 'gy'), may hold values from 0 to 127
- marine_point_switch: int32 [1024, 512], P('gx', 'gy'), may hold values 0 or 1
- potential_heat_deviation: float32 [8, 1024, 512], P(None, 'gx', 'gy'), may hold values from -6 to 6
- free_marine_lift: float32 [1024, 512], P('gx', 'gy'), may hold values from -3 to 3
- depth_averaged_uflow: float32 [1024, 512], P('gx', 'gy'), may hold values from -3 to 3
- depth_averaged_vflow: float32 [1024, 512], P('gx', 'gy'), may hold values from -3 to 3
Outputs:
- atmo_skin_temp_back: float32 [384, 1024], P('gy', 'gx')
- ocean_temp_after_step: float32 [8, 1024, 512], P(None, 'gx', 'gy')
- barotropic: float32 [3, 1024, 512], P(None, 'gx', 'gy')
The draws below stay inside these ranges and needn't reach their ends.
Inputs may be any that keep to these rules, and one draw needn't show every extreme that they name: `piece_keeper_part`: ocean devices are counted with gx slowest. Among the 96 blocks of one atmosphere device at most 6 have the same owner, and some device has exactly 6 with one owner; every ocean device owns some block.
All inputs are finite; a program needn't handle non-finite values. No bound on the sum of `marine_point_switch` on one device may be relied on, other than what follows from the above.
Results may differ from the reference program's by a relative error of at most 0.0026.
Values may be sent and summed in bfloat16 or wider, within the bound.
A program may use at most 64 MiB of HBM per device.

```python
import math
import jax
import jax.numpy as jnp
import numpy as np

NB = 96
BA = 128
OX = 128
BAND_NORTH_COUNT = 128
MARINE_STRATA = 8
SUB = 40
CAP = 6
ATMO_NS_TOTAL = 384
ATMO_EW_TOTAL = 1024
OCEANIC_EW_TOTAL = 1024
MARINE_LAT_SPAN = 512
N_GX = 8
N_GY = 4


def plant(values, stream_key, smallest, largest):
    place = [jax.random.randint(jax.random.fold_in(stream_key, axis), (), 0, length) for axis, length in enumerate(values.shape)]
    longest = values.shape.index(max(values.shape))
    next_to = place[:longest] + [(place[longest] + 1) % values.shape[longest]] + place[longest + 1:]
    return values.at[tuple(place)].set(smallest).at[tuple(next_to)].set(largest)


def block_levels(key, shape, split, least, top_value):
    def one(dim, parts):
        heights = jax.random.uniform(jax.random.fold_in(jax.random.fold_in(key, 6), dim), (parts,), jnp.float32, least / len(split), top_value / len(split))
        return jnp.repeat(jnp.exp(heights), shape[dim] // parts).reshape((-1,) + (1,) * (len(shape) - dim - 1))

    factor_of = one(*split[0])
    for cut in split[1:]:
        factor_of = factor_of * one(*cut)
    return factor_of


def assign_block(own_key, own, number, rows, count, top, limit, slope):
    sequence = jax.random.permutation(own_key, count)
    crowded, ordinary = portions_of(count, rows * top, limit, slope, True), portions_of(count, rows * top, limit, slope, False)
    places = jnp.arange(count)

    def named(sizes, turn):
        used = int((sizes > 0).sum())
        fixed = max(1, used // 4)
        passed = fixed + (places - fixed + turn * (used - fixed)) % max(1, count - fixed)
        return jnp.zeros((count,), jnp.int32).at[sequence[jnp.where(places < fixed, places, passed)]].set(jnp.asarray(sizes, jnp.int32))

    sizes = jnp.where(number % 4 == 0, named(crowded, number // 4), named(ordinary, number - number // 4 - 1))
    mixed = jax.random.permutation(jax.random.fold_in(own, 3), count)
    donor, taker = mixed[0:count // 2 * 2:2], mixed[1:count // 2 * 2:2]
    margin = jnp.minimum(sizes[donor] - 1, limit - sizes[taker]) // 2
    margin = jnp.where((donor == sequence[0]) | (taker == sequence[0]) | (sizes[taker] == 0), 0, jnp.maximum(margin, 0))
    passed = jax.random.randint(jax.random.fold_in(own, 4), (count // 2,), 0, 1 << 20) % (margin + 1)
    sizes = sizes.at[donor].add(-passed).at[taker].add(passed)
    items = jnp.searchsorted(jnp.cumsum(sizes), jnp.arange(rows * top), side="right").astype(jnp.int32)
    grid = items.reshape(top, rows).T
    grid = grid[jax.random.permutation(jax.random.fold_in(own, 1), rows)]
    turn = jax.random.randint(jax.random.fold_in(own, 2), (rows, 1), 0, top)
    return jnp.take_along_axis(grid, (jnp.arange(top)[None, :] + turn) % top, axis=1)


def portions_of(number_of, total, reach, slope, full):
    loads = [(1 << 20) // math.isqrt(rank ** slope) + 1 for rank in range(1, number_of + 1)]
    largest = reach if full else min(reach, max(-(-total // number_of), total * loads[0] // sum(loads)))
    least = 1 if total - largest >= number_of - 1 else 0
    counts, rest = [largest] + [least] * (number_of - 1), total - largest - least * (number_of - 1)
    while rest > 0:
        movable = [i for i in range(1, number_of) if counts[i] < largest] or [i for i in range(1, number_of) if counts[i] < reach]
        mass, budget = sum([loads[i] for i in movable]), rest
        for i in movable:
            addition = min(reach - counts[i], max(1, budget * loads[i] // mass), rest)
            counts[i] = counts[i] + addition
            rest = rest - addition
    return np.array(counts)


def bell_draw(stream_key, shape, scale, limit, split=(), kind=jnp.bfloat16):
    gain = block_levels(stream_key, shape, split, -0.22, 0.18) if split else 1.0
    entries = jax.random.normal(stream_key, shape, jnp.float32) * scale * gain
    return jnp.minimum(jnp.maximum(entries, -limit), limit).astype(kind)


def setup_inputs(seed: int = 0) -> dict:
    seeds = jax.random.split(jax.random.key(seed), 10)
    sky_interface_transfers = bell_draw(seeds[0], (4, ATMO_NS_TOTAL, ATMO_EW_TOTAL), 1.0, 6.0, ((1, 4), (2, 8)))
    coupling_matrix_enlarged = bell_draw(seeds[1], (ATMO_NS_TOTAL, ATMO_EW_TOTAL, BAND_NORTH_COUNT), BA ** -0.5, 0.5, ((0, 4), (1, 8)))
    piece_keeper_part_keys = jax.random.split(jax.random.fold_in(seeds[2], 1), N_GX * ATMO_NS_TOTAL // NB)
    piece_keeper_part_turns = jax.random.permutation(jax.random.fold_in(seeds[2], 3), N_GX * ATMO_NS_TOTAL // NB)
    piece_keeper_part = jax.vmap(lambda own, number: assign_block(jax.random.fold_in(seeds[2], 2), own, number, NB, N_GX * N_GY, 1, CAP, 2))(piece_keeper_part_keys, piece_keeper_part_turns).reshape((N_GX, ATMO_NS_TOTAL, 1))
    receiving_part_line = plant(jax.random.randint(seeds[3], (N_GX, ATMO_NS_TOTAL), 0, OX), jax.random.fold_in(seeds[3], 1), 0, OX - 1).astype(jnp.int32)
    marine_point_switch = plant((jax.random.randint(seeds[4], (OCEANIC_EW_TOTAL, MARINE_LAT_SPAN), 0, 8) < 7).astype(jnp.int32), jax.random.fold_in(seeds[4], 1), 0, 1)
    potential_heat_deviation = bell_draw(seeds[5], (MARINE_STRATA, OCEANIC_EW_TOTAL, MARINE_LAT_SPAN), 1.0, 6.0, ((1, 8), (2, 4)), jnp.float32)
    free_marine_lift = bell_draw(seeds[6], (OCEANIC_EW_TOTAL, MARINE_LAT_SPAN), 0.5, 3.0, ((0, 8), (1, 4)), jnp.float32)
    depth_averaged_uflow = bell_draw(seeds[7], (OCEANIC_EW_TOTAL, MARINE_LAT_SPAN), 0.5, 3.0, ((0, 8), (1, 4)), jnp.float32)
    depth_averaged_vflow = bell_draw(seeds[8], (OCEANIC_EW_TOTAL, MARINE_LAT_SPAN), 0.5, 3.0, ((0, 8), (1, 4)), jnp.float32)
    return {"sky_interface_transfers": sky_interface_transfers, "coupling_matrix_enlarged": coupling_matrix_enlarged, "piece_keeper_part": piece_keeper_part, "receiving_part_line": receiving_part_line, "marine_point_switch": marine_point_switch, "potential_heat_deviation": potential_heat_deviation, "free_marine_lift": free_marine_lift, "depth_averaged_uflow": depth_averaged_uflow, "depth_averaged_vflow": depth_averaged_vflow}


HORIZ_MIX = 0.15
VERT_MIX = 0.2
HEAT_GAIN = 0.5
FLOW_DAMP = 0.98
PRESS_GAIN = 0.6
DIVERGE_GAIN = 0.6
CORIOLIS = 0.1
WIND_GAIN = 0.05
FRESH_GAIN = 0.05


def velocity(height_rim, east_flow_component, north_flow_component, stress_east, stress_north, turning, liquid_portion):
    slope_east = height_rim[2:, 1:-1] - height_rim[:-2, 1:-1]
    slope_north = height_rim[1:-1, 2:] - height_rim[1:-1, :-2]
    zonal_new = (FLOW_DAMP * east_flow_component - PRESS_GAIN * slope_east + turning * north_flow_component + WIND_GAIN * stress_east) * liquid_portion
    merid_new = (FLOW_DAMP * north_flow_component - PRESS_GAIN * slope_north - turning * zonal_new + WIND_GAIN * stress_north) * liquid_portion
    return zonal_new, merid_new


def height(oceanic_top_sheet, zonal_rim, merid_rim, fresh_in, liquid_portion):
    spread = (zonal_rim[2:, 1:-1] - zonal_rim[:-2, 1:-1]) + (merid_rim[1:-1, 2:] - merid_rim[1:-1, :-2])
    return (oceanic_top_sheet - DIVERGE_GAIN * spread - FRESH_GAIN * fresh_in) * liquid_portion


def integrate_scalar_once(heat_deviation, heat_deviation_fringe, liquid_portion_fringe, incoming_enthalpy, liquid_portion):
    horizontal_diffusion = liquid_portion_fringe[2:, 1:-1] * (heat_deviation_fringe[:, 2:, 1:-1] - heat_deviation)
    horizontal_diffusion = horizontal_diffusion + liquid_portion_fringe[:-2, 1:-1] * (heat_deviation_fringe[:, :-2, 1:-1] - heat_deviation)
    horizontal_diffusion = horizontal_diffusion + liquid_portion_fringe[1:-1, 2:] * (heat_deviation_fringe[:, 1:-1, 2:] - heat_deviation)
    horizontal_diffusion = horizontal_diffusion + liquid_portion_fringe[1:-1, :-2] * (heat_deviation_fringe[:, 1:-1, :-2] - heat_deviation)
    above_level = jnp.concatenate([heat_deviation[:1], heat_deviation[:-1]], axis=0)
    below_level = jnp.concatenate([heat_deviation[1:], heat_deviation[-1:]], axis=0)
    vertical = (above_level - heat_deviation) + (below_level - heat_deviation)
    tendency = heat_deviation + HORIZ_MIX * horizontal_diffusion + VERT_MIX * vertical
    tendency = tendency.at[0].add(HEAT_GAIN * incoming_enthalpy)
    return tendency * liquid_portion


def reference(sky_interface_transfers, coupling_matrix_enlarged, piece_keeper_part, receiving_part_line, marine_point_switch, potential_heat_deviation, free_marine_lift, depth_averaged_uflow, depth_averaged_vflow):
    flux_blocks = sky_interface_transfers.astype(jnp.float32).reshape(4, ATMO_NS_TOTAL, N_GX, BA)
    subdomain_regrid_operator = coupling_matrix_enlarged.astype(jnp.float32).reshape(ATMO_NS_TOTAL, N_GX, BA, BAND_NORTH_COUNT)
    pieces = jnp.einsum("frgc,rgco->grfo", flux_blocks, subdomain_regrid_operator)
    target = piece_keeper_part[:, :, 0]
    flattened_sequence = (((target // N_GY) * OX + receiving_part_line) * N_GY + target % N_GY).astype(jnp.int32)
    collected = jnp.zeros((OCEANIC_EW_TOTAL * N_GY, 4, BAND_NORTH_COUNT), jnp.float32).at[flattened_sequence.reshape(-1)].add(pieces.reshape(-1, 4, BAND_NORTH_COUNT))
    marine_interface_transfers = collected.reshape(OCEANIC_EW_TOTAL, N_GY, 4, BAND_NORTH_COUNT).transpose(2, 0, 1, 3).reshape(4, OCEANIC_EW_TOTAL, MARINE_LAT_SPAN)
    rows_sea = jnp.arange(MARINE_LAT_SPAN, dtype=jnp.int32)
    wall_mask = ((rows_sea > 0) & (rows_sea < MARINE_LAT_SPAN - 1)).astype(jnp.float32)
    liquid_portion = marine_point_switch.astype(jnp.float32) * wall_mask[None, :]
    heat_deviation_fringe = jnp.pad(potential_heat_deviation, ((0, 0), (1, 1), (1, 1)), mode="wrap")
    liquid_portion_fringe = jnp.pad(liquid_portion, 1, mode="wrap")
    ocean_temp_after_step = integrate_scalar_once(potential_heat_deviation, heat_deviation_fringe, liquid_portion_fringe, marine_interface_transfers[2], liquid_portion)
    turning = CORIOLIS * jnp.sin(jnp.pi * ((rows_sea.astype(jnp.float32) + 0.5) / MARINE_LAT_SPAN - 0.5))[None, :]
    oceanic_top_sheet = free_marine_lift
    east_flow_component = depth_averaged_uflow
    north_flow_component = depth_averaged_vflow
    for substep in range(SUB):
        east_flow_component, north_flow_component = velocity(jnp.pad(oceanic_top_sheet, 1, mode="wrap"), east_flow_component, north_flow_component, marine_interface_transfers[0], marine_interface_transfers[1], turning, liquid_portion)
        flow_rim = jnp.pad(jnp.stack([east_flow_component, north_flow_component]), ((0, 0), (1, 1), (1, 1)), mode="wrap")
        oceanic_top_sheet = height(oceanic_top_sheet, flow_rim[0], flow_rim[1], marine_interface_transfers[3], liquid_portion)
    coupled_skin_warmness = ocean_temp_after_step[0].astype(jnp.bfloat16).reshape(OCEANIC_EW_TOTAL * N_GY, BAND_NORTH_COUNT)
    coupled_skin_warmness_band = coupled_skin_warmness[flattened_sequence]
    atmo_skin_temp_back = jnp.einsum("lpgm,plm->lpg", subdomain_regrid_operator, coupled_skin_warmness_band.astype(jnp.float32)).reshape(ATMO_NS_TOTAL, ATMO_EW_TOTAL)
    return atmo_skin_temp_back, ocean_temp_after_step, jnp.stack([oceanic_top_sheet, east_flow_component, north_flow_component])
```

```python
import jax
import jax.numpy as jnp
from jax import lax
from jax.experimental import pallas as pl
from jax.experimental.pallas import tpu as pltpu
from jax.sharding import PartitionSpec as P

NB = 96
OX = 128
BAND_NORTH_COUNT = 128
MARINE_STRATA = 8
SUB = 40


HORIZ_MIX = 0.15
VERT_MIX = 0.2
HEAT_GAIN = 0.5
FLOW_DAMP = 0.98
PRESS_GAIN = 0.6
DIVERGE_GAIN = 0.6
CORIOLIS = 0.1
WIND_GAIN = 0.05
FRESH_GAIN = 0.05


def padded(x, sides, width):
    for axis, dim in sides:
        size, length = (lax.axis_size(axis), x.shape[dim])
        up = [(i, (i + 1) % size) for i in range(size)]
        down = [(j, i) for i, j in up]
        last = lax.slice_in_dim(x, length - width, length, axis=dim)
        first = lax.slice_in_dim(x, 0, width, axis=dim)
        before = lax.ppermute(last, axis, up)
        after = lax.ppermute(first, axis, down)
        x = jnp.concatenate([before, x, after], axis=dim)
    return x


MESH = pl.DeviceIdType.MESH
HALF = BAND_NORTH_COUNT // 2
WIDE = OX + 2 * HALF
PACK = HALF // 2
SPAN = SUB // 2
CHUNK = 16


def low_lanes(rows):
    return lax.broadcasted_iota(jnp.int32, (rows, BAND_NORTH_COUNT), 1) < HALF


def pack_half(values):
    low = low_lanes(PACK)
    first, second = values[:PACK], pltpu.roll(values[PACK:], HALF, 1)
    return (
        jnp.where(low, first, second).astype(jnp.bfloat16),
        jnp.where(low, second, first).astype(jnp.bfloat16),
    )


def unpack_half(low_quadrant, high_quadrant):
    low = low_lanes(PACK)
    lo = low_quadrant.astype(jnp.float32)
    hi = high_quadrant.astype(jnp.float32)
    return jnp.where(low, lo, hi), pltpu.roll(jnp.where(low, hi, lo), HALF, 1)


def neighbours():
    nx, ny = lax.axis_size("gx"), lax.axis_size("gy")
    x, y = lax.axis_index("gx"), lax.axis_index("gy")
    up, down = lax.rem(x + 1, nx), lax.rem(x + nx - 1, nx)
    right, left = lax.rem(y + 1, ny), lax.rem(y + ny - 1, ny)
    return x, y, up, down, right, left


def greet():
    x, y, up, down, right, left = neighbours()
    barrier = pltpu.get_barrier_semaphore()
    for place in (
        (up, y),
        (down, y),
        (x, right),
        (x, left),
        (up, right),
        (up, left),
        (down, right),
        (down, left),
    ):
        pl.semaphore_signal(barrier, inc=1, device_id=place, device_id_type=MESH)
    pl.semaphore_wait(barrier, 8)


def margin_copies(quads, edge, side, send_sem, recv_sem):
    x, y, up, down, right, left = neighbours()
    plan = (
        (quads.at[1], edge.at[0], (up, y)),
        (quads.at[0], edge.at[1], (down, y)),
        (quads.at[0, 1], side.at[1, 1], (x, right)),
        (quads.at[1, 1], side.at[2, 1], (x, right)),
        (quads.at[0, 0], side.at[1, 0], (x, left)),
        (quads.at[1, 0], side.at[2, 0], (x, left)),
        (quads.at[1, 1], side.at[0, 1], (up, right)),
        (quads.at[1, 0], side.at[0, 0], (up, left)),
        (quads.at[0, 1], side.at[3, 1], (down, right)),
        (quads.at[0, 0], side.at[3, 0], (down, left)),
    )
    return [
        pltpu.make_async_remote_copy(
            src_ref=src,
            dst_ref=dst,
            send_sem=send_sem.at[k],
            recv_sem=recv_sem.at[k],
            device_id=place,
            device_id_type=MESH,
        )
        for k, (src, dst, place) in enumerate(plan)
    ]


def fill_quads(quads, field, values):
    for part in range(2):
        lo, hi = pack_half(values[part * HALF : (part + 1) * HALF])
        quads[part, 0, field] = lo
        quads[part, 1, field] = hi


def spread_margin(edge, side, field, wide):
    for row_block in range(4):
        start = row_block * HALF
        if row_block in (0, 3):
            at = 0 if row_block == 0 else 1
            one, two = unpack_half(edge[at, 0, field], edge[at, 1, field])
            wide[0, start : start + PACK] = one
            wide[0, start + PACK : start + HALF] = two
        one, two = unpack_half(side[row_block, 0, field], side[row_block, 1, field])
        wide[1, start : start + PACK] = one
        wide[1, start + PACK : start + HALF] = two


def lat_difference(own, far):
    lane = lax.broadcasted_iota(jnp.int32, own.shape, 1)
    last, first = lane == BAND_NORTH_COUNT - 1, lane == 0
    own_up = pltpu.roll(own, BAND_NORTH_COUNT - 1, 1)
    far_up = pltpu.roll(far, BAND_NORTH_COUNT - 1, 1)
    own_down = pltpu.roll(own, 1, 1)
    far_down = pltpu.roll(far, 1, 1)
    return (
        jnp.where(last, far_up, own_up) - jnp.where(first, far_down, own_down),
        jnp.where(last, own_up, far_up) - jnp.where(first, own_down, far_down),
    )


def substep(reach, h, u, v, east, north, fresh, wet, turning):
    low, high = HALF - reach, HALF + OX + reach
    turn = [
        jnp.broadcast_to(turning[tile : tile + 1, :], (CHUNK, BAND_NORTH_COUNT))
        for tile in range(2)
    ]
    for start in range(low, high, CHUNK):
        rows = slice(start, start + CHUNK)
        slope_north = lat_difference(h[0, rows], h[1, rows])
        for tile in range(2):
            slope_east = (
                h[tile, start + 1 : start + CHUNK + 1] - h[tile, start - 1 : start + CHUNK - 1]
            )
            old_u, old_v, mask = u[tile, rows], v[tile, rows], wet[tile, rows]
            new_u = (
                FLOW_DAMP * old_u - PRESS_GAIN * slope_east + turn[tile] * old_v + east[tile, rows]
            ) * mask
            u[tile, rows] = new_u
            v[tile, rows] = (
                FLOW_DAMP * old_v
                - PRESS_GAIN * slope_north[tile]
                - turn[tile] * new_u
                + north[tile, rows]
            ) * mask
    for start in range(low, high, CHUNK):
        rows = slice(start, start + CHUNK)
        spread_north = lat_difference(v[0, rows], v[1, rows])
        for tile in range(2):
            spread_east = (
                u[tile, start + 1 : start + CHUNK + 1] - u[tile, start - 1 : start + CHUNK - 1]
            )
            h[tile, rows] = (
                h[tile, rows]
                - DIVERGE_GAIN * (spread_east + spread_north[tile])
                - fresh[tile, rows]
            ) * wet[tile, rows]


def run_span(h, u, v, east, north, fresh, wet, turning):
    done = 0
    while done < SPAN:
        need = 2 * (SPAN - done) - 1
        reach = -(-need // 8) * 8
        steps = min(SPAN - done, 4)

        def one(_, carry, reach=reach):
            substep(reach, h, u, v, east, north, fresh, wet, turning)
            return carry

        lax.fori_loop(0, steps, one, 0)
        done += steps


def flow_kernel(
    h_in, u_in, v_in, e_in, n_in, f_in, w_in, turning, out,
    wide, quads1, edge1, side1, quads2, edge2, side2,
    send1, recv1, send2, recv2,
):
    fields = (h_in, u_in, v_in, e_in, n_in, f_in, w_in)
    gains = (None, None, None, WIND_GAIN, WIND_GAIN, FRESH_GAIN, None)
    greet()
    for k, (ref, gain) in enumerate(zip(fields, gains)):
        values = ref[...] if gain is None else gain * ref[...]
        wide[k, 0, HALF : HALF + OX] = values
        fill_quads(quads1, k, values)
    copies = margin_copies(quads1, edge1, side1, send1, recv1)
    for copy in copies:
        copy.start()
    for copy in copies:
        copy.wait()
    for k in range(7):
        spread_margin(edge1, side1, k, wide.at[k])
    parts = [wide.at[k] for k in range(7)]
    run_span(*parts, turning)
    for k in range(3):
        fill_quads(quads2, k, wide[k, 0, HALF : HALF + OX])
    copies = margin_copies(quads2, edge2, side2, send2, recv2)
    for copy in copies:
        copy.start()
    for copy in copies:
        copy.wait()
    for k in range(3):
        spread_margin(edge2, side2, k, wide.at[k])
    run_span(*parts, turning)
    for k in range(3):
        out[k] = wide[k, 0, HALF : HALF + OX]


def turning_rows():
    total_y = lax.axis_size("gy") * BAND_NORTH_COUNT
    lane = jnp.arange(BAND_NORTH_COUNT, dtype=jnp.int32)
    own = lax.axis_index("gy") * BAND_NORTH_COUNT + lane
    far = jnp.where(lane < HALF, own + BAND_NORTH_COUNT, own - BAND_NORTH_COUNT)
    rows = jnp.mod(jnp.stack([own, far]), total_y)
    return CORIOLIS * jnp.sin(jnp.pi * ((rows.astype(jnp.float32) + 0.5) / total_y - 0.5))


def flow(h, u, v, east, north, fresh, wet):
    def boxes(count):
        return [
            pltpu.VMEM((2, 2, count, PACK, BAND_NORTH_COUNT), jnp.bfloat16),
            pltpu.VMEM((2, 2, count, PACK, BAND_NORTH_COUNT), jnp.bfloat16),
            pltpu.VMEM((4, 2, count, PACK, BAND_NORTH_COUNT), jnp.bfloat16),
        ]

    return pl.pallas_call(
        flow_kernel,
        out_shape=jax.ShapeDtypeStruct((3, OX, BAND_NORTH_COUNT), jnp.float32),
        in_specs=[pl.BlockSpec(memory_space=pltpu.VMEM)] * 8,
        out_specs=pl.BlockSpec(memory_space=pltpu.VMEM),
        scratch_shapes=[pltpu.VMEM((7, 2, WIDE, BAND_NORTH_COUNT), jnp.float32)]
        + boxes(7)
        + boxes(3)
        + [pltpu.SemaphoreType.DMA((10,))] * 4,
        compiler_params=pltpu.CompilerParams(collective_id=0, has_side_effects=True),
        name="flow",
    )(h, u, v, east, north, fresh, wet, turning_rows())


def integrate_scalar_once(
    heat_deviation, heat_deviation_fringe, liquid_portion_fringe, incoming_enthalpy, liquid_portion
):
    horizontal_diffusion = liquid_portion_fringe[2:, 1:-1] * (
        heat_deviation_fringe[:, 2:, 1:-1] - heat_deviation
    )
    horizontal_diffusion = horizontal_diffusion + liquid_portion_fringe[:-2, 1:-1] * (
        heat_deviation_fringe[:, :-2, 1:-1] - heat_deviation
    )
    horizontal_diffusion = horizontal_diffusion + liquid_portion_fringe[1:-1, 2:] * (
        heat_deviation_fringe[:, 1:-1, 2:] - heat_deviation
    )
    horizontal_diffusion = horizontal_diffusion + liquid_portion_fringe[1:-1, :-2] * (
        heat_deviation_fringe[:, 1:-1, :-2] - heat_deviation
    )
    above_level = jnp.concatenate([heat_deviation[:1], heat_deviation[:-1]], axis=0)
    below_level = jnp.concatenate([heat_deviation[1:], heat_deviation[-1:]], axis=0)
    vertical = above_level - heat_deviation + (below_level - heat_deviation)
    tendency = heat_deviation + HORIZ_MIX * horizontal_diffusion + VERT_MIX * vertical
    tendency = tendency.at[0].add(HEAT_GAIN * incoming_enthalpy)
    return tendency * liquid_portion


def per_device(
    sky_interface_transfers,
    coupling_matrix_enlarged,
    piece_keeper_part,
    receiving_part_line,
    marine_point_switch,
    potential_heat_deviation,
    free_marine_lift,
    depth_averaged_uflow,
    depth_averaged_vflow,
):
    width_x = lax.axis_size("gx")
    width_y = lax.axis_size("gy")
    worker_groups = width_x * width_y
    greatest_entries = max(2, 2 * NB // worker_groups)
    slot_count = worker_groups * greatest_entries
    partial_value = jnp.einsum(
        "fnc,nco->nfo",
        sky_interface_transfers,
        coupling_matrix_enlarged,
        preferred_element_type=jnp.float32,
    )
    target = piece_keeper_part[0, :, 0]
    hit_table = (target[:, None] == jnp.arange(worker_groups, dtype=jnp.int32)[None, :]).astype(
        jnp.int32
    )
    before = jnp.cumsum(hit_table, axis=0) - hit_table
    slot_index = target * greatest_entries + jnp.sum(before * hit_table, axis=1)
    chosen = slot_index[None, :] == jnp.arange(slot_count, dtype=jnp.int32)[:, None]
    packed = jnp.einsum(
        "sn,nfo->sfo", chosen.astype(jnp.float32), partial_value, precision=lax.Precision.HIGHEST
    )
    rows_sent = jnp.sum(chosen.astype(jnp.int32) * receiving_part_line[0][None, :], axis=1)
    arrived, rows_got = (
        lax.all_to_all(
            packed.reshape(worker_groups, greatest_entries, 4, BAND_NORTH_COUNT),
            ("gx", "gy"),
            split_axis=0,
            concat_axis=0,
            tiled=True,
        ),
        lax.all_to_all(
            rows_sent.reshape(worker_groups, greatest_entries),
            ("gx", "gy"),
            split_axis=0,
            concat_axis=0,
            tiled=True,
        ),
    )
    arrived = arrived.reshape(slot_count, 4, BAND_NORTH_COUNT)
    rows_got = rows_got.reshape(slot_count)
    arrival_place = rows_got[:, None] == jnp.arange(OX, dtype=jnp.int32)[None, :]
    marine_interface_transfers = jnp.einsum(
        "sx,sfo->fxo", arrival_place.astype(jnp.float32), arrived, precision=lax.Precision.HIGHEST
    )
    total_y = width_y * BAND_NORTH_COUNT
    rows_sea = lax.axis_index("gy") * BAND_NORTH_COUNT + jnp.arange(
        BAND_NORTH_COUNT, dtype=jnp.int32
    )
    wall_mask = ((rows_sea > 0) & (rows_sea < total_y - 1)).astype(jnp.float32)
    liquid_portion = marine_point_switch.astype(jnp.float32) * wall_mask[None, :]
    gathered_pieces = jnp.concatenate([potential_heat_deviation, liquid_portion[None]], axis=0)
    with_halo_cells = padded(gathered_pieces, (("gx", 1), ("gy", 2)), 1)
    ocean_temp_after_step = integrate_scalar_once(
        potential_heat_deviation,
        with_halo_cells[:MARINE_STRATA],
        with_halo_cells[MARINE_STRATA],
        marine_interface_transfers[2],
        liquid_portion,
    )
    coupled_skin_warmness = ocean_temp_after_step[0].astype(jnp.bfloat16)
    coupled_skin_warmness_band = jnp.dot(
        arrival_place.astype(jnp.bfloat16),
        coupled_skin_warmness,
        preferred_element_type=jnp.float32,
    ).astype(jnp.bfloat16)
    skin_back = lax.all_to_all(
        coupled_skin_warmness_band.reshape(worker_groups, greatest_entries, BAND_NORTH_COUNT),
        ("gx", "gy"),
        split_axis=0,
        concat_axis=0,
        tiled=True,
    )
    skin_mine = jnp.einsum(
        "sn,so->no",
        chosen.astype(jnp.bfloat16),
        skin_back.reshape(slot_count, BAND_NORTH_COUNT),
        preferred_element_type=jnp.float32,
    ).astype(jnp.bfloat16)
    atmo_skin_temp_back = jnp.einsum(
        "nco,no->nc", coupling_matrix_enlarged, skin_mine, preferred_element_type=jnp.float32
    )
    barotropic = flow(
        free_marine_lift,
        depth_averaged_uflow,
        depth_averaged_vflow,
        marine_interface_transfers[0],
        marine_interface_transfers[1],
        marine_interface_transfers[3],
        liquid_portion,
    )
    return (atmo_skin_temp_back, ocean_temp_after_step, barotropic)


def solution(mesh):
    in_specs = (
        P(None, "gy", "gx"),
        P("gy", "gx", None),
        P("gx", "gy", None),
        P("gx", "gy"),
        P("gx", "gy"),
        P(None, "gx", "gy"),
        P("gx", "gy"),
        P("gx", "gy"),
        P("gx", "gy"),
    )
    out_specs = (P("gy", "gx"), P(None, "gx", "gy"), P(None, "gx", "gy"))
    return jax.shard_map(
        per_device, mesh=mesh, in_specs=in_specs, out_specs=out_specs, check_vma=False
    )
```

```python
import jax
import jax.numpy as jnp
from jax import lax
from jax.experimental import pallas as pl
from jax.experimental.pallas import tpu as pltpu
from jax.sharding import PartitionSpec as P

NB = 96
OX = 128
BAND_NORTH_COUNT = 128
MARINE_STRATA = 8
SUB = 40


HORIZ_MIX = 0.15
VERT_MIX = 0.2
HEAT_GAIN = 0.5
FLOW_DAMP = 0.98
PRESS_GAIN = 0.6
DIVERGE_GAIN = 0.6
CORIOLIS = 0.1
WIND_GAIN = 0.05
FRESH_GAIN = 0.05


MESH = pl.DeviceIdType.MESH
HALF = BAND_NORTH_COUNT // 2
WIDE = OX + 2 * HALF
PACK = HALF // 2
SPAN = SUB // 2
CHUNK = 16
SLOTS = 8


def low_lanes(rows):
    return lax.broadcasted_iota(jnp.int32, (rows, BAND_NORTH_COUNT), 1) < HALF


def pack_half(values):
    low = low_lanes(PACK)
    first, second = values[:PACK], pltpu.roll(values[PACK:], HALF, 1)
    return (
        jnp.where(low, first, second).astype(jnp.bfloat16),
        jnp.where(low, second, first).astype(jnp.bfloat16),
    )


def unpack_half(low_quadrant, high_quadrant):
    low = low_lanes(PACK)
    lo = low_quadrant.astype(jnp.float32)
    hi = high_quadrant.astype(jnp.float32)
    return jnp.where(low, lo, hi), pltpu.roll(jnp.where(low, hi, lo), HALF, 1)


def neighbours():
    nx, ny = lax.axis_size("gx"), lax.axis_size("gy")
    x, y = lax.axis_index("gx"), lax.axis_index("gy")
    up, down = lax.rem(x + 1, nx), lax.rem(x + nx - 1, nx)
    right, left = lax.rem(y + 1, ny), lax.rem(y + ny - 1, ny)
    return x, y, up, down, right, left


def peer_place(index):
    ny = lax.axis_size("gy")
    return lax.div(index, ny), lax.rem(index, ny)


def greet_all(me, count):
    barrier = pltpu.get_barrier_semaphore()

    def one(k, carry):
        place = peer_place(lax.rem(me + k, count))
        pl.semaphore_signal(barrier, inc=1, device_id=place, device_id_type=MESH)
        return carry

    lax.fori_loop(1, count, one, 0)


def swap_all(action, me, count, out, into, send_sem, recv_sem):
    def one(k, carry):
        peer = lax.rem(me + k, count)
        copy = pltpu.make_async_remote_copy(
            src_ref=out.at[peer],
            dst_ref=into.at[me],
            send_sem=send_sem.at[k],
            recv_sem=recv_sem.at[k],
            device_id=peer_place(peer),
            device_id_type=MESH,
        )
        if action == "start":
            copy.start()
        else:
            copy.wait()
        return carry

    lax.fori_loop(1, count, one, 0)


def as_bits(condition):
    return jnp.where(condition, 1.0, 0.0).astype(jnp.bfloat16)


def line_numbers(shape, axis):
    return lax.broadcasted_iota(jnp.int32, shape, axis).astype(jnp.float32)


def dot(a, b, a_dim=1, b_dim=0):
    return lax.dot_general(
        a, b, (((a_dim,), (b_dim,)), ((), ())), preferred_element_type=jnp.float32
    )


def place_blocks(keeper, lines, count):
    i, j = line_numbers((NB, NB), 0), line_numbers((NB, NB), 1)
    owner_col = keeper[...].astype(jnp.float32)
    owner_row = jnp.sum(jnp.where(i == j, owner_col, 0.0), axis=0, keepdims=True)
    same = jnp.where(owner_col == owner_row, 1.0, 0.0)
    rank_row = jnp.sum(jnp.where(i < j, same, 0.0), axis=0, keepdims=True)
    rank_col = jnp.sum(jnp.where(j < i, same, 0.0), axis=1, keepdims=True)
    line_row = lines[...].astype(jnp.float32)
    line_col = jnp.sum(jnp.where(i == j, line_row, 0.0), axis=1, keepdims=True)
    hot = as_bits(line_numbers((NB, OX), 1) == line_col)
    key_row = owner_row * SLOTS + rank_row
    key_col = owner_col * SLOTS + rank_col
    return key_row, rank_row, key_col, hot


def fill_send(send, partial, key_row, rank_row, hot, count, most):
    spare = SLOTS - most
    place = line_numbers((count * SLOTS, NB), 0)
    slots = as_bits(place == key_row)
    out = []
    for f in range(4):
        value = dot(slots, partial[f].astype(jnp.bfloat16))
        if f * spare < most:
            here = (rank_row >= f * spare) & (rank_row < (f + 1) * spare)
            spot = jnp.where(here, key_row - f * spare + most, -1.0)
            value = value + dot(as_bits(place == spot), hot)
        out.append(value.reshape(count, SLOTS, BAND_NORTH_COUNT))
    for p in range(2):
        both = jnp.concatenate([out[2 * p], out[2 * p + 1]], axis=1)
        send[:, 2 * SLOTS * p : 2 * SLOTS * (p + 1), :] = both.astype(jnp.bfloat16)


def read_received(recv, count, most):
    spare = SLOTS - most
    total = count * SLOTS
    values = []
    for p in range(2):
        both = recv[:, 2 * SLOTS * p : 2 * SLOTS * (p + 1), :].astype(jnp.float32)
        values.append(both[:, :SLOTS].reshape(total, BAND_NORTH_COUNT))
        values.append(both[:, SLOTS:].reshape(total, BAND_NORTH_COUNT))
    slot = lax.broadcasted_iota(jnp.int32, (count, SLOTS, BAND_NORTH_COUNT), 1)
    slot = slot.reshape(total, BAND_NORTH_COUNT)
    target = jnp.zeros((total, BAND_NORTH_COUNT), jnp.float32)
    for f in range(4):
        if f * spare < most:
            moved = pltpu.roll(values[f], total - (most - f * spare), 0)
            here = (slot >= f * spare) & (slot < min((f + 1) * spare, most))
            target = jnp.where(here, moved, target)
    return [value.astype(jnp.bfloat16) for value in values], target


def edge_selector(rows, low_row, high_row):
    row = lax.broadcasted_iota(jnp.int32, (rows, BAND_NORTH_COUNT), 0)
    lane = lax.broadcasted_iota(jnp.int32, (rows, BAND_NORTH_COUNT), 1)
    return as_bits(
        ((row == low_row) & (lane == 0)) | ((row == high_row) & (lane == BAND_NORTH_COUNT - 1))
    )


def fill_heat_edges(heat, edges):
    selector = edge_selector(8, 0, 1)
    for k in range(MARINE_STRATA):
        level = slice(k, k + 1)
        edges[0, level] = heat[k, 0:1]
        edges[1, level] = heat[k, OX - 1 : OX]
        sides = dot(selector, heat[k].astype(jnp.bfloat16), 1, 1)
        edges[2, level] = sides[0:1]
        edges[3, level] = sides[1:2]


def heat_copies(edges, got, send_sem, recv_sem):
    x, y, up, down, right, left = neighbours()
    plan = ((1, 0, (up, y)), (0, 1, (down, y)), (3, 2, (x, right)), (2, 3, (x, left)))
    return [
        pltpu.make_async_remote_copy(
            src_ref=edges.at[src],
            dst_ref=got.at[dst],
            send_sem=send_sem.at[k],
            recv_sem=recv_sem.at[k],
            device_id=place,
            device_id_type=MESH,
        )
        for k, (src, dst, place) in enumerate(plan)
    ]


def heat_step(heat, got, tall, wet, near, out):
    own = slice(HALF, HALF + OX)
    last = lax.broadcasted_iota(jnp.int32, (OX, BAND_NORTH_COUNT), 1) == BAND_NORTH_COUNT - 1
    first = lax.broadcasted_iota(jnp.int32, (OX, BAND_NORTH_COUNT), 1) == 0
    mine, far = wet[0, own], wet[1, own]
    near[0] = jnp.where(last, pltpu.roll(far, OX - 1, 1), pltpu.roll(mine, OX - 1, 1))
    near[1] = jnp.where(first, pltpu.roll(far, 1, 1), pltpu.roll(mine, 1, 1))
    sides = jnp.concatenate([got[3], got[2]], axis=0).astype(jnp.bfloat16)
    for k in range(MARINE_STRATA):
        tall[k, 8 : 8 + OX] = heat[k]
        tall[k, 7:8] = got[0, k : k + 1]
        tall[k, 8 + OX : 9 + OX] = got[1, k : k + 1]
        near[2 + k] = dot(sides, edge_selector(2 * MARINE_STRATA, MARINE_STRATA + k, k), 0, 0)

    step = 32
    last, first = last[:step], first[:step]

    def one(k, carry):
        above, below = jnp.maximum(k - 1, 0), jnp.minimum(k + 1, MARINE_STRATA - 1)
        for start in range(0, OX, step):
            rows = slice(start, start + step)
            wide_rows = lambda shift: slice(HALF + start + shift, HALF + start + step + shift)
            here = heat[k, rows]
            side = near[2 + k, rows]
            north = jnp.where(last, side, pltpu.roll(here, OX - 1, 1))
            south = jnp.where(first, side, pltpu.roll(here, 1, 1))
            lateral = wet[0, wide_rows(1)] * (tall[k, 9 + start : 9 + start + step] - here)
            lateral = lateral + wet[0, wide_rows(-1)] * (
                tall[k, 7 + start : 7 + start + step] - here
            )
            lateral = lateral + near[0, rows] * (north - here)
            lateral = lateral + near[1, rows] * (south - here)
            vertical = (heat[above, rows] - here) + (heat[below, rows] - here)
            out[k, rows] = (here + HORIZ_MIX * lateral + VERT_MIX * vertical) * wet[0, wide_rows(0)]
        return carry

    lax.fori_loop(0, MARINE_STRATA, one, 0)


def margin_copies(quads, edge, side, send_sem, recv_sem):
    x, y, up, down, right, left = neighbours()
    plan = (
        (quads.at[1], edge.at[0], (up, y)),
        (quads.at[0], edge.at[1], (down, y)),
        (quads.at[0, 1], side.at[1, 1], (x, right)),
        (quads.at[1, 1], side.at[2, 1], (x, right)),
        (quads.at[0, 0], side.at[1, 0], (x, left)),
        (quads.at[1, 0], side.at[2, 0], (x, left)),
        (quads.at[1, 1], side.at[0, 1], (up, right)),
        (quads.at[1, 0], side.at[0, 0], (up, left)),
        (quads.at[0, 1], side.at[3, 1], (down, right)),
        (quads.at[0, 0], side.at[3, 0], (down, left)),
    )
    return [
        pltpu.make_async_remote_copy(
            src_ref=src,
            dst_ref=dst,
            send_sem=send_sem.at[k],
            recv_sem=recv_sem.at[k],
            device_id=place,
            device_id_type=MESH,
        )
        for k, (src, dst, place) in enumerate(plan)
    ]


def fill_quads(quads, field, values):
    for part in range(2):
        lo, hi = pack_half(values[part * HALF : (part + 1) * HALF])
        quads[part, 0, field] = lo
        quads[part, 1, field] = hi


def spread_margin(edge, side, field, wide):
    for row_block in range(4):
        start = row_block * HALF
        if row_block in (0, 3):
            at = 0 if row_block == 0 else 1
            one, two = unpack_half(edge[at, 0, field], edge[at, 1, field])
            wide[0, start : start + PACK] = one
            wide[0, start + PACK : start + HALF] = two
        one, two = unpack_half(side[row_block, 0, field], side[row_block, 1, field])
        wide[1, start : start + PACK] = one
        wide[1, start + PACK : start + HALF] = two


def lat_difference(own, far):
    lane = lax.broadcasted_iota(jnp.int32, own.shape, 1)
    last, first = lane == BAND_NORTH_COUNT - 1, lane == 0
    own_up = pltpu.roll(own, BAND_NORTH_COUNT - 1, 1)
    far_up = pltpu.roll(far, BAND_NORTH_COUNT - 1, 1)
    own_down = pltpu.roll(own, 1, 1)
    far_down = pltpu.roll(far, 1, 1)
    return (
        jnp.where(last, far_up, own_up) - jnp.where(first, far_down, own_down),
        jnp.where(last, own_up, far_up) - jnp.where(first, own_down, far_down),
    )


def substep(reach, h, u, v, east, north, fresh, wet, turning):
    low, high = HALF - reach, HALF + OX + reach
    turn = [
        jnp.broadcast_to(turning[tile : tile + 1, :], (CHUNK, BAND_NORTH_COUNT))
        for tile in range(2)
    ]
    for start in range(low, high, CHUNK):
        rows = slice(start, start + CHUNK)
        slope_north = lat_difference(h[0, rows], h[1, rows])
        for tile in range(2):
            slope_east = (
                h[tile, start + 1 : start + CHUNK + 1] - h[tile, start - 1 : start + CHUNK - 1]
            )
            old_u, old_v, mask = u[tile, rows], v[tile, rows], wet[tile, rows]
            new_u = (
                FLOW_DAMP * old_u - PRESS_GAIN * slope_east + turn[tile] * old_v + east[tile, rows]
            ) * mask
            u[tile, rows] = new_u
            v[tile, rows] = (
                FLOW_DAMP * old_v
                - PRESS_GAIN * slope_north[tile]
                - turn[tile] * new_u
                + north[tile, rows]
            ) * mask
    for start in range(low, high, CHUNK):
        rows = slice(start, start + CHUNK)
        spread_north = lat_difference(v[0, rows], v[1, rows])
        for tile in range(2):
            spread_east = (
                u[tile, start + 1 : start + CHUNK + 1] - u[tile, start - 1 : start + CHUNK - 1]
            )
            h[tile, rows] = (
                h[tile, rows]
                - DIVERGE_GAIN * (spread_east + spread_north[tile])
                - fresh[tile, rows]
            ) * wet[tile, rows]


def run_span(h, u, v, east, north, fresh, wet, turning):
    done = 0
    while done < SPAN:
        need = 2 * (SPAN - done) - 1
        reach = -(-need // 8) * 8
        steps = min(SPAN - done, 4)

        def one(_, carry, reach=reach):
            substep(reach, h, u, v, east, north, fresh, wet, turning)
            return carry

        lax.fori_loop(0, steps, one, 0)
        done += steps


def window_kernel(
    sky, weights_far, keeper, lines, sea, heat, h_in, u_in, v_in, turning,
    back, heat_out, out,
    weights, sky32, partial, send, recv, skin_send, skin_recv,
    heat_edges, heat_got, tall, near,
    wide, quads1, edge1, side1, quads2, edge2, side2, quads3, edge3, side3,
    load_sem, a2a_send, a2a_recv, skin_send_sem, skin_recv_sem,
    heat_send_sem, heat_recv_sem, send1, recv1, send2, recv2, send3, recv3,
):
    ny = lax.axis_size("gy")
    count = lax.axis_size("gx") * ny
    most = max(2, 2 * NB // count)
    me = lax.axis_index("gx") * ny + lax.axis_index("gy")
    own = slice(HALF, HALF + OX)
    greet_all(me, count)
    load = pltpu.make_async_copy(weights_far, weights, load_sem)
    load.start()
    lat = lax.axis_index("gy") * BAND_NORTH_COUNT + lax.broadcasted_iota(
        jnp.int32, (OX, BAND_NORTH_COUNT), 1
    )
    inside = (lat > 0) & (lat < ny * BAND_NORTH_COUNT - 1)
    mask = jnp.where(inside, sea[...].astype(jnp.float32), 0.0)
    for k, values in enumerate((h_in[...], u_in[...], v_in[...], mask)):
        wide[k, 0, own] = values
        fill_quads(quads1, k, values)
    fill_heat_edges(heat, heat_edges)
    sky32[...] = sky[...].astype(jnp.float32)
    key_row, rank_row, key_col, hot = place_blocks(keeper, lines, count)
    pl.semaphore_wait(pltpu.get_barrier_semaphore(), count - 1)
    copies1 = margin_copies(quads1, edge1, side1, send1, recv1)
    heats = heat_copies(heat_edges, heat_got, heat_send_sem, heat_recv_sem)
    for copy in copies1 + heats:
        copy.start()
    load.wait()
    slot32 = lax.rem(
        lax.broadcasted_iota(jnp.int32, (4 * SLOTS, BAND_NORTH_COUNT), 0), SLOTS
    )
    for g in range(NB // SLOTS):
        rows = slice(g * SLOTS, (g + 1) * SLOTS)
        fluxes = sky32[:, rows, :].reshape(4 * SLOTS, OX).astype(jnp.bfloat16)
        total = dot(fluxes, weights[g * SLOTS])
        for n in range(1, SLOTS):
            total = jnp.where(slot32 == n, dot(fluxes, weights[g * SLOTS + n]), total)
        partial[:, rows, :] = total.reshape(4, SLOTS, BAND_NORTH_COUNT)
    fill_send(send, partial, key_row, rank_row, hot, count, most)
    swap_all("start", me, count, send, recv, a2a_send, a2a_recv)
    recv[me] = send[me]
    for copy in copies1 + heats:
        copy.wait()
    for k in range(4):
        spread_margin(edge1, side1, k, wide.at[k])
    heat_step(heat, heat_got, tall, wide.at[3], near, heat_out)
    swap_all("wait", me, count, send, recv, a2a_send, a2a_recv)
    values, target = read_received(recv, count, most)
    target_turned = target.T.astype(jnp.bfloat16)
    target = target.astype(jnp.bfloat16)
    for k, (f, gain) in enumerate(((0, WIND_GAIN), (1, WIND_GAIN), (3, FRESH_GAIN))):
        flux = gain * dot(target_turned, values[f])
        wide[4 + k, 0, own] = flux
        fill_quads(quads2, k, flux)
    copies2 = margin_copies(quads2, edge2, side2, send2, recv2)
    for copy in copies2:
        copy.start()
    surface = heat_out[0] + HEAT_GAIN * dot(target_turned, values[2]) * wide[3, 0, own]
    heat_out[0] = surface
    band = dot(target, surface.astype(jnp.bfloat16))
    skin_send[...] = band.reshape(count, SLOTS, BAND_NORTH_COUNT)
    swap_all("start", me, count, skin_send, skin_recv, skin_send_sem, skin_recv_sem)
    skin_recv[me] = skin_send[me]
    for copy in copies2:
        copy.wait()
    for k in range(3):
        spread_margin(edge2, side2, k, wide.at[4 + k])
    parts = [wide.at[k] for k in (0, 1, 2, 4, 5, 6, 3)]
    run_span(*parts, turning)
    for k in range(3):
        fill_quads(quads3, k, wide[k, 0, own])
    copies3 = margin_copies(quads3, edge3, side3, send3, recv3)
    for copy in copies3:
        copy.start()
    swap_all("wait", me, count, skin_send, skin_recv, skin_send_sem, skin_recv_sem)
    slots = as_bits(line_numbers((NB, count * SLOTS), 1) == key_col)
    skin = dot(slots, skin_recv[...].reshape(count * SLOTS, BAND_NORTH_COUNT).astype(jnp.bfloat16))
    slot8 = lax.broadcasted_iota(jnp.int32, (SLOTS, BAND_NORTH_COUNT), 0)
    for g in range(NB // SLOTS):
        rows = slice(g * SLOTS, (g + 1) * SLOTS)
        lines_skin = skin[rows].astype(jnp.bfloat16)
        total = dot(lines_skin, weights[g * SLOTS], 1, 1)
        for n in range(1, SLOTS):
            total = jnp.where(slot8 == n, dot(lines_skin, weights[g * SLOTS + n], 1, 1), total)
        back[rows] = total
    for copy in copies3:
        copy.wait()
    for k in range(3):
        spread_margin(edge3, side3, k, wide.at[k])
    run_span(*parts, turning)
    for k in range(3):
        out[k] = wide[k, 0, own]


def turning_rows():
    total_y = lax.axis_size("gy") * BAND_NORTH_COUNT
    lane = jnp.arange(BAND_NORTH_COUNT, dtype=jnp.int32)
    own = lax.axis_index("gy") * BAND_NORTH_COUNT + lane
    far = jnp.where(lane < HALF, own + BAND_NORTH_COUNT, own - BAND_NORTH_COUNT)
    rows = jnp.mod(jnp.stack([own, far]), total_y)
    return CORIOLIS * jnp.sin(jnp.pi * ((rows.astype(jnp.float32) + 0.5) / total_y - 0.5))


def per_device(
    sky_interface_transfers,
    coupling_matrix_enlarged,
    piece_keeper_part,
    receiving_part_line,
    marine_point_switch,
    potential_heat_deviation,
    free_marine_lift,
    depth_averaged_uflow,
    depth_averaged_vflow,
):
    count = lax.axis_size("gx") * lax.axis_size("gy")
    line = BAND_NORTH_COUNT

    def boxes(fields):
        return [
            pltpu.VMEM((2, 2, fields, PACK, line), jnp.bfloat16),
            pltpu.VMEM((2, 2, fields, PACK, line), jnp.bfloat16),
            pltpu.VMEM((4, 2, fields, PACK, line), jnp.bfloat16),
        ]

    inside = pl.BlockSpec(memory_space=pltpu.VMEM)
    return pl.pallas_call(
        window_kernel,
        out_shape=(
            jax.ShapeDtypeStruct((NB, OX), jnp.float32),
            jax.ShapeDtypeStruct((MARINE_STRATA, OX, line), jnp.float32),
            jax.ShapeDtypeStruct((3, OX, line), jnp.float32),
        ),
        in_specs=[inside, pl.BlockSpec(memory_space=pl.ANY)] + [inside] * 8,
        out_specs=(inside,) * 3,
        scratch_shapes=[
            pltpu.VMEM((NB, OX, line), jnp.bfloat16),
            pltpu.VMEM((4, NB, OX), jnp.float32),
            pltpu.VMEM((4, NB, line), jnp.float32),
            pltpu.VMEM((count, 4 * SLOTS, line), jnp.bfloat16),
            pltpu.VMEM((count, 4 * SLOTS, line), jnp.bfloat16),
            pltpu.VMEM((count, SLOTS, line), jnp.float32),
            pltpu.VMEM((count, SLOTS, line), jnp.float32),
            pltpu.VMEM((4, MARINE_STRATA, line), jnp.float32),
            pltpu.VMEM((4, MARINE_STRATA, line), jnp.float32),
            pltpu.VMEM((MARINE_STRATA, OX + 16, line), jnp.float32),
            pltpu.VMEM((2 + MARINE_STRATA, OX, line), jnp.float32),
            pltpu.VMEM((7, 2, WIDE, line), jnp.float32),
        ]
        + boxes(4)
        + boxes(3)
        + boxes(3)
        + [pltpu.SemaphoreType.DMA]
        + [pltpu.SemaphoreType.DMA((count,))] * 4
        + [pltpu.SemaphoreType.DMA((4,))] * 2
        + [pltpu.SemaphoreType.DMA((10,))] * 6,
        compiler_params=pltpu.CompilerParams(collective_id=0, has_side_effects=True),
        name="window",
    )(
        sky_interface_transfers,
        coupling_matrix_enlarged,
        piece_keeper_part.reshape(NB, 1),
        receiving_part_line,
        marine_point_switch,
        potential_heat_deviation,
        free_marine_lift,
        depth_averaged_uflow,
        depth_averaged_vflow,
        turning_rows(),
    )


def solution(mesh):
    in_specs = (
        P(None, "gy", "gx"),
        P("gy", "gx", None),
        P("gx", "gy", None),
        P("gx", "gy"),
        P("gx", "gy"),
        P(None, "gx", "gy"),
        P("gx", "gy"),
        P("gx", "gy"),
        P("gx", "gy"),
    )
    out_specs = (P("gy", "gx"), P(None, "gx", "gy"), P(None, "gx", "gy"))
    return jax.shard_map(
        per_device, mesh=mesh, in_specs=in_specs, out_specs=out_specs, check_vma=False
    )
```

```python
import jax
import jax.numpy as jnp
from jax import lax
from jax.experimental import pallas as pl
from jax.experimental.pallas import tpu as pltpu
from jax.sharding import PartitionSpec as P

NB = 96
OX = 128
BAND_NORTH_COUNT = 128
MARINE_STRATA = 8
SUB = 40


HORIZ_MIX = 0.15
VERT_MIX = 0.2
HEAT_GAIN = 0.5
FLOW_DAMP = 0.98
PRESS_GAIN = 0.6
DIVERGE_GAIN = 0.6
CORIOLIS = 0.1
WIND_GAIN = 0.05
FRESH_GAIN = 0.05


MESH = pl.DeviceIdType.MESH
HALF = BAND_NORTH_COUNT // 2
WIDE = OX + 2 * HALF
PACK = HALF // 2
SPAN = SUB // 2
CHUNK = 16
SLOTS = 8
FLUXES = 5


def low_lanes(rows):
    return lax.broadcasted_iota(jnp.int32, (rows, BAND_NORTH_COUNT), 1) < HALF


def pack_half(values):
    low = low_lanes(PACK)
    first, second = values[:PACK], pltpu.roll(values[PACK:], HALF, 1)
    return (
        jnp.where(low, first, second).astype(jnp.bfloat16),
        jnp.where(low, second, first).astype(jnp.bfloat16),
    )


def unpack_half(low_quadrant, high_quadrant):
    low = low_lanes(PACK)
    lo = low_quadrant.astype(jnp.float32)
    hi = high_quadrant.astype(jnp.float32)
    return jnp.where(low, lo, hi), pltpu.roll(jnp.where(low, hi, lo), HALF, 1)


def neighbours():
    nx, ny = lax.axis_size("gx"), lax.axis_size("gy")
    x, y = lax.axis_index("gx"), lax.axis_index("gy")
    up, down = lax.rem(x + 1, nx), lax.rem(x + nx - 1, nx)
    right, left = lax.rem(y + 1, ny), lax.rem(y + ny - 1, ny)
    return x, y, up, down, right, left


def peer_place(index):
    ny = lax.axis_size("gy")
    return lax.div(index, ny), lax.rem(index, ny)


def greet_all(me, count):
    barrier = pltpu.get_barrier_semaphore()

    def one(k, carry):
        place = peer_place(lax.rem(me + k, count))
        pl.semaphore_signal(barrier, inc=1, device_id=place, device_id_type=MESH)
        return carry

    lax.fori_loop(1, count, one, 0)


def swap_all(action, me, count, out, into, send_sem, recv_sem):
    def one(k, carry):
        peer = lax.rem(me + k, count)
        copy = pltpu.make_async_remote_copy(
            src_ref=out.at[peer],
            dst_ref=into.at[me],
            send_sem=send_sem.at[k],
            recv_sem=recv_sem.at[k],
            device_id=peer_place(peer),
            device_id_type=MESH,
        )
        if action == "start":
            copy.start()
        else:
            copy.wait()
        return carry

    lax.fori_loop(1, count, one, 0)


def as_bits(condition):
    return jnp.where(condition, 1.0, 0.0).astype(jnp.bfloat16)


def line_numbers(shape, axis):
    return lax.broadcasted_iota(jnp.int32, shape, axis).astype(jnp.float32)


def dot(a, b, a_dim=1, b_dim=0):
    return lax.dot_general(
        a, b, (((a_dim,), (b_dim,)), ((), ())), preferred_element_type=jnp.float32
    )


def place_blocks(keeper, lines, count):
    i, j = line_numbers((NB, NB), 0), line_numbers((NB, NB), 1)
    owner_row = keeper[...].astype(jnp.float32)
    owner_col = jnp.sum(jnp.where(i == j, owner_row, 0.0), axis=1, keepdims=True)
    same = jnp.where(owner_col == owner_row, 1.0, 0.0)
    rank_row = jnp.sum(jnp.where(i < j, same, 0.0), axis=0, keepdims=True)
    rank_col = jnp.sum(jnp.where(j < i, same, 0.0), axis=1, keepdims=True)
    line_row = lines[...].astype(jnp.float32)
    line_col = jnp.sum(jnp.where(i == j, line_row, 0.0), axis=1, keepdims=True)
    hot = as_bits(line_numbers((NB, OX), 1) == line_col)
    key_row = owner_row * SLOTS + rank_row
    key_col = owner_col * SLOTS + rank_col
    return key_row, rank_row, key_col, hot


def fill_send(send, partial, key_row, rank_row, hot, count, most):
    spare = SLOTS - most
    place = line_numbers((count * SLOTS, NB), 0)
    slots = as_bits(place == key_row)
    out = []
    heat_flux = partial[2]
    heat_high = heat_flux.astype(jnp.bfloat16)
    heat_low = (heat_flux - heat_high.astype(jnp.float32)).astype(jnp.bfloat16)
    sources = [partial[f].astype(jnp.bfloat16) for f in range(4)]
    sources = sources[:2] + [heat_high, sources[3], heat_low]
    for f in range(FLUXES):
        value = dot(slots, sources[f])
        if f * spare < most:
            here = (rank_row >= f * spare) & (rank_row < (f + 1) * spare)
            spot = jnp.where(here, key_row - f * spare + most, -1.0)
            value = value + dot(as_bits(place == spot), hot)
        out.append(value.reshape(count, SLOTS, BAND_NORTH_COUNT))
    out.append(jnp.zeros_like(out[0]))
    for p in range(3):
        both = jnp.concatenate([out[2 * p], out[2 * p + 1]], axis=1)
        send[:, 2 * SLOTS * p : 2 * SLOTS * (p + 1), :] = both.astype(jnp.bfloat16)


def read_received(recv, count, most):
    spare = SLOTS - most
    total = count * SLOTS
    values = []
    for p in range(3):
        both = recv[:, 2 * SLOTS * p : 2 * SLOTS * (p + 1), :].astype(jnp.float32)
        values.append(both[:, :SLOTS].reshape(total, BAND_NORTH_COUNT))
        values.append(both[:, SLOTS:].reshape(total, BAND_NORTH_COUNT))
    slot = lax.broadcasted_iota(jnp.int32, (count, SLOTS, BAND_NORTH_COUNT), 1)
    slot = slot.reshape(total, BAND_NORTH_COUNT)
    target = jnp.zeros((total, BAND_NORTH_COUNT), jnp.float32)
    for f in range(FLUXES):
        if f * spare < most:
            moved = pltpu.roll(values[f], total - (most - f * spare), 0)
            here = (slot >= f * spare) & (slot < min((f + 1) * spare, most))
            target = jnp.where(here, moved, target)
    return [value.astype(jnp.bfloat16) for value in values], target


def edge_selector(rows, low_row, high_row):
    row = lax.broadcasted_iota(jnp.int32, (rows, BAND_NORTH_COUNT), 0)
    lane = lax.broadcasted_iota(jnp.int32, (rows, BAND_NORTH_COUNT), 1)
    return as_bits(
        ((row == low_row) & (lane == 0)) | ((row == high_row) & (lane == BAND_NORTH_COUNT - 1))
    )


def fill_heat_edges(heat, edges):
    selector = edge_selector(8, 0, 1)
    for k in range(MARINE_STRATA):
        level = slice(k, k + 1)
        edges[0, level] = heat[k, 0:1]
        edges[1, level] = heat[k, OX - 1 : OX]
        sides = dot(selector, heat[k].astype(jnp.bfloat16), 1, 1)
        edges[2, level] = sides[0:1]
        edges[3, level] = sides[1:2]


def heat_copies(edges, got, send_sem, recv_sem):
    x, y, up, down, right, left = neighbours()
    plan = ((1, 0, (up, y)), (0, 1, (down, y)), (3, 2, (x, right)), (2, 3, (x, left)))
    return [
        pltpu.make_async_remote_copy(
            src_ref=edges.at[src],
            dst_ref=got.at[dst],
            send_sem=send_sem.at[k],
            recv_sem=recv_sem.at[k],
            device_id=place,
            device_id_type=MESH,
        )
        for k, (src, dst, place) in enumerate(plan)
    ]


def heat_step(heat, got, tall, wet, near, out):
    own = slice(HALF, HALF + OX)
    last = lax.broadcasted_iota(jnp.int32, (OX, BAND_NORTH_COUNT), 1) == BAND_NORTH_COUNT - 1
    first = lax.broadcasted_iota(jnp.int32, (OX, BAND_NORTH_COUNT), 1) == 0
    mine, far = wet[0, own], wet[1, own]
    near[0] = jnp.where(last, pltpu.roll(far, OX - 1, 1), pltpu.roll(mine, OX - 1, 1))
    near[1] = jnp.where(first, pltpu.roll(far, 1, 1), pltpu.roll(mine, 1, 1))
    sides = jnp.concatenate([got[3], got[2]], axis=0).astype(jnp.bfloat16)
    for k in range(MARINE_STRATA):
        tall[k, 8 : 8 + OX] = heat[k]
        tall[k, 7:8] = got[0, k : k + 1]
        tall[k, 8 + OX : 9 + OX] = got[1, k : k + 1]
        near[2 + k] = dot(sides, edge_selector(2 * MARINE_STRATA, MARINE_STRATA + k, k), 0, 0)

    step = 32
    last, first = last[:step], first[:step]

    def one(k, carry):
        above, below = jnp.maximum(k - 1, 0), jnp.minimum(k + 1, MARINE_STRATA - 1)
        for start in range(0, OX, step):
            rows = slice(start, start + step)
            wide_rows = lambda shift: slice(HALF + start + shift, HALF + start + step + shift)
            here = heat[k, rows]
            side = near[2 + k, rows]
            north = jnp.where(last, side, pltpu.roll(here, OX - 1, 1))
            south = jnp.where(first, side, pltpu.roll(here, 1, 1))
            lateral = wet[0, wide_rows(1)] * (tall[k, 9 + start : 9 + start + step] - here)
            lateral = lateral + wet[0, wide_rows(-1)] * (
                tall[k, 7 + start : 7 + start + step] - here
            )
            lateral = lateral + near[0, rows] * (north - here)
            lateral = lateral + near[1, rows] * (south - here)
            vertical = (heat[above, rows] - here) + (heat[below, rows] - here)
            out[k, rows] = (here + HORIZ_MIX * lateral + VERT_MIX * vertical) * wet[0, wide_rows(0)]
        return carry

    lax.fori_loop(0, MARINE_STRATA, one, 0)


def margin_copies(quads, edge, side, send_sem, recv_sem):
    x, y, up, down, right, left = neighbours()
    plan = (
        (quads.at[1], edge.at[0], (up, y)),
        (quads.at[0], edge.at[1], (down, y)),
        (quads.at[0, 1], side.at[1, 1], (x, right)),
        (quads.at[1, 1], side.at[2, 1], (x, right)),
        (quads.at[0, 0], side.at[1, 0], (x, left)),
        (quads.at[1, 0], side.at[2, 0], (x, left)),
        (quads.at[1, 1], side.at[0, 1], (up, right)),
        (quads.at[1, 0], side.at[0, 0], (up, left)),
        (quads.at[0, 1], side.at[3, 1], (down, right)),
        (quads.at[0, 0], side.at[3, 0], (down, left)),
    )
    return [
        pltpu.make_async_remote_copy(
            src_ref=src,
            dst_ref=dst,
            send_sem=send_sem.at[k],
            recv_sem=recv_sem.at[k],
            device_id=place,
            device_id_type=MESH,
        )
        for k, (src, dst, place) in enumerate(plan)
    ]


def fill_quads(quads, field, values):
    for part in range(2):
        lo, hi = pack_half(values[part * HALF : (part + 1) * HALF])
        quads[part, 0, field] = lo
        quads[part, 1, field] = hi


def spread_margin(edge, side, field, wide):
    for row_block in range(4):
        start = row_block * HALF
        if row_block in (0, 3):
            at = 0 if row_block == 0 else 1
            one, two = unpack_half(edge[at, 0, field], edge[at, 1, field])
            wide[0, start : start + PACK] = one
            wide[0, start + PACK : start + HALF] = two
        one, two = unpack_half(side[row_block, 0, field], side[row_block, 1, field])
        wide[1, start : start + PACK] = one
        wide[1, start + PACK : start + HALF] = two


def lat_difference(own, far):
    lane = lax.broadcasted_iota(jnp.int32, own.shape, 1)
    last, first = lane == BAND_NORTH_COUNT - 1, lane == 0
    own_up = pltpu.roll(own, BAND_NORTH_COUNT - 1, 1)
    far_up = pltpu.roll(far, BAND_NORTH_COUNT - 1, 1)
    own_down = pltpu.roll(own, 1, 1)
    far_down = pltpu.roll(far, 1, 1)
    return (
        jnp.where(last, far_up, own_up) - jnp.where(first, far_down, own_down),
        jnp.where(last, own_up, far_up) - jnp.where(first, own_down, far_down),
    )


def substep(reach, h, u, v, east, north, fresh, wet, turning):
    low, high = HALF - reach, HALF + OX + reach
    turn = [
        jnp.broadcast_to(turning[tile : tile + 1, :], (CHUNK, BAND_NORTH_COUNT))
        for tile in range(2)
    ]
    for start in range(low, high, CHUNK):
        rows = slice(start, start + CHUNK)
        slope_north = lat_difference(h[0, rows], h[1, rows])
        for tile in range(2):
            slope_east = (
                h[tile, start + 1 : start + CHUNK + 1] - h[tile, start - 1 : start + CHUNK - 1]
            )
            old_u, old_v, mask = u[tile, rows], v[tile, rows], wet[tile, rows]
            new_u = (
                FLOW_DAMP * old_u - PRESS_GAIN * slope_east + turn[tile] * old_v + east[tile, rows]
            ) * mask
            u[tile, rows] = new_u
            v[tile, rows] = (
                FLOW_DAMP * old_v
                - PRESS_GAIN * slope_north[tile]
                - turn[tile] * new_u
                + north[tile, rows]
            ) * mask
    for start in range(low, high, CHUNK):
        rows = slice(start, start + CHUNK)
        spread_north = lat_difference(v[0, rows], v[1, rows])
        for tile in range(2):
            spread_east = (
                u[tile, start + 1 : start + CHUNK + 1] - u[tile, start - 1 : start + CHUNK - 1]
            )
            h[tile, rows] = (
                h[tile, rows]
                - DIVERGE_GAIN * (spread_east + spread_north[tile])
                - fresh[tile, rows]
            ) * wet[tile, rows]


def run_span(h, u, v, east, north, fresh, wet, turning):
    done = 0
    while done < SPAN:
        need = 2 * (SPAN - done) - 1
        reach = -(-need // 8) * 8
        steps = min(SPAN - done, 4)

        def one(_, carry, reach=reach):
            substep(reach, h, u, v, east, north, fresh, wet, turning)
            return carry

        lax.fori_loop(0, steps, one, 0)
        done += steps


def window_kernel(
    sky, weights_far, keeper, lines, sea, heat, h_in, u_in, v_in,
    back, heat_out, out,
    turning, weights, sky32, partial, send, recv, skin_send, skin_recv,
    heat_edges, heat_got, tall, near,
    wide, quads1, edge1, side1, quads2, edge2, side2, quads3, edge3, side3,
    load_sem, a2a_send, a2a_recv, skin_send_sem, skin_recv_sem,
    heat_send_sem, heat_recv_sem, send1, recv1, send2, recv2, send3, recv3,
):
    ny = lax.axis_size("gy")
    count = lax.axis_size("gx") * ny
    most = max(2, 2 * NB // count)
    me = lax.axis_index("gx") * ny + lax.axis_index("gy")
    own = slice(HALF, HALF + OX)
    greet_all(me, count)
    turning[...] = turning_rows()
    load = pltpu.make_async_copy(weights_far, weights, load_sem)
    load.start()
    lat = lax.axis_index("gy") * BAND_NORTH_COUNT + lax.broadcasted_iota(
        jnp.int32, (OX, BAND_NORTH_COUNT), 1
    )
    inside = (lat > 0) & (lat < ny * BAND_NORTH_COUNT - 1)
    mask = jnp.where(inside, sea[...].astype(jnp.float32), 0.0)
    for k, values in enumerate((h_in[...], u_in[...], v_in[...], mask)):
        wide[k, 0, own] = values
        fill_quads(quads1, k, values)
    fill_heat_edges(heat, heat_edges)
    sky32[...] = sky[...].astype(jnp.float32)
    key_row, rank_row, key_col, hot = place_blocks(keeper, lines, count)
    pl.semaphore_wait(pltpu.get_barrier_semaphore(), count - 1)
    copies1 = margin_copies(quads1, edge1, side1, send1, recv1)
    heats = heat_copies(heat_edges, heat_got, heat_send_sem, heat_recv_sem)
    for copy in copies1 + heats:
        copy.start()
    load.wait()
    slot32 = lax.rem(
        lax.broadcasted_iota(jnp.int32, (4 * SLOTS, BAND_NORTH_COUNT), 0), SLOTS
    )
    for g in range(NB // SLOTS):
        rows = slice(g * SLOTS, (g + 1) * SLOTS)
        fluxes = sky32[:, rows, :].reshape(4 * SLOTS, OX).astype(jnp.bfloat16)
        total = dot(fluxes, weights[g * SLOTS])
        for n in range(1, SLOTS):
            total = jnp.where(slot32 == n, dot(fluxes, weights[g * SLOTS + n]), total)
        partial[:, rows, :] = total.reshape(4, SLOTS, BAND_NORTH_COUNT)
    fill_send(send, partial, key_row, rank_row, hot, count, most)
    swap_all("start", me, count, send, recv, a2a_send, a2a_recv)
    recv[me] = send[me]
    for copy in copies1 + heats:
        copy.wait()
    for k in range(4):
        spread_margin(edge1, side1, k, wide.at[k])
    heat_step(heat, heat_got, tall, wide.at[3], near, heat_out)
    swap_all("wait", me, count, send, recv, a2a_send, a2a_recv)
    values, target = read_received(recv, count, most)
    target_turned = target.T.astype(jnp.bfloat16)
    target = target.astype(jnp.bfloat16)
    for k, (f, gain) in enumerate(((0, WIND_GAIN), (1, WIND_GAIN), (3, FRESH_GAIN))):
        flux = gain * dot(target_turned, values[f])
        wide[4 + k, 0, own] = flux
        fill_quads(quads2, k, flux)
    copies2 = margin_copies(quads2, edge2, side2, send2, recv2)
    for copy in copies2:
        copy.start()
    heat_flux = dot(target_turned, values[2]) + dot(target_turned, values[4])
    surface = heat_out[0] + HEAT_GAIN * heat_flux * wide[3, 0, own]
    heat_out[0] = surface
    band = dot(target, surface.astype(jnp.bfloat16))
    skin_send[...] = band.reshape(count, SLOTS, BAND_NORTH_COUNT)
    swap_all("start", me, count, skin_send, skin_recv, skin_send_sem, skin_recv_sem)
    skin_recv[me] = skin_send[me]
    for copy in copies2:
        copy.wait()
    for k in range(3):
        spread_margin(edge2, side2, k, wide.at[4 + k])
    parts = [wide.at[k] for k in (0, 1, 2, 4, 5, 6, 3)]
    run_span(*parts, turning)
    for k in range(3):
        fill_quads(quads3, k, wide[k, 0, own])
    copies3 = margin_copies(quads3, edge3, side3, send3, recv3)
    for copy in copies3:
        copy.start()
    swap_all("wait", me, count, skin_send, skin_recv, skin_send_sem, skin_recv_sem)
    slots = as_bits(line_numbers((NB, count * SLOTS), 1) == key_col)
    skin = dot(slots, skin_recv[...].reshape(count * SLOTS, BAND_NORTH_COUNT).astype(jnp.bfloat16))
    slot8 = lax.broadcasted_iota(jnp.int32, (SLOTS, BAND_NORTH_COUNT), 0)
    for g in range(NB // SLOTS):
        rows = slice(g * SLOTS, (g + 1) * SLOTS)
        lines_skin = skin[rows].astype(jnp.bfloat16)
        total = dot(lines_skin, weights[g * SLOTS], 1, 1)
        for n in range(1, SLOTS):
            total = jnp.where(slot8 == n, dot(lines_skin, weights[g * SLOTS + n], 1, 1), total)
        back[rows] = total
    for copy in copies3:
        copy.wait()
    for k in range(3):
        spread_margin(edge3, side3, k, wide.at[k])
    run_span(*parts, turning)
    for k in range(3):
        out[k] = wide[k, 0, own]


def turning_rows():
    total_y = lax.axis_size("gy") * BAND_NORTH_COUNT
    shape = (8, BAND_NORTH_COUNT)
    lane = lax.broadcasted_iota(jnp.int32, shape, 1)
    tile = lax.broadcasted_iota(jnp.int32, shape, 0)
    away = jnp.where(lane < HALF, BAND_NORTH_COUNT, -BAND_NORTH_COUNT)
    rows = lax.axis_index("gy") * BAND_NORTH_COUNT + lane + jnp.where(tile == 0, 0, away)
    rows = jnp.where(rows < 0, rows + total_y, jnp.where(rows < total_y, rows, rows - total_y))
    return CORIOLIS * jnp.sin(jnp.pi * ((rows.astype(jnp.float32) + 0.5) / total_y - 0.5))


def hand_over(*refs):
    sources, targets = refs[:3], refs[3:6]
    buffers, loads, stores = refs[6:9], refs[9], refs[10]
    into = [
        pltpu.make_async_copy(sources[k], buffers[k], loads.at[k]) for k in range(3)
    ]
    away = [
        pltpu.make_async_copy(buffers[k], targets[k], stores.at[k]) for k in range(3)
    ]
    for copy in into:
        copy.start()
    for k in range(3):
        into[k].wait()
        away[k].start()
    for copy in away:
        copy.wait()


def per_device(
    sky_interface_transfers,
    coupling_matrix_enlarged,
    piece_keeper_part,
    receiving_part_line,
    marine_point_switch,
    potential_heat_deviation,
    free_marine_lift,
    depth_averaged_uflow,
    depth_averaged_vflow,
):
    count = lax.axis_size("gx") * lax.axis_size("gy")
    line = BAND_NORTH_COUNT

    def boxes(fields):
        return [
            pltpu.VMEM((2, 2, fields, PACK, line), jnp.bfloat16),
            pltpu.VMEM((2, 2, fields, PACK, line), jnp.bfloat16),
            pltpu.VMEM((4, 2, fields, PACK, line), jnp.bfloat16),
        ]

    inside = pl.BlockSpec(memory_space=pltpu.VMEM)
    shapes = (
            jax.ShapeDtypeStruct((NB, OX), jnp.float32),
            jax.ShapeDtypeStruct((MARINE_STRATA, OX, line), jnp.float32),
            jax.ShapeDtypeStruct((3, OX, line), jnp.float32),
        )
    results = pl.pallas_call(
        window_kernel,
        out_shape=shapes,
        in_specs=[inside, pl.BlockSpec(memory_space=pl.ANY)] + [inside] * 7,
        out_specs=(inside,) * 3,
        scratch_shapes=[
            pltpu.VMEM((8, line), jnp.float32),
            pltpu.VMEM((NB, OX, line), jnp.bfloat16),
            pltpu.VMEM((4, NB, OX), jnp.float32),
            pltpu.VMEM((4, NB, line), jnp.float32),
            pltpu.VMEM((count, 6 * SLOTS, line), jnp.bfloat16),
            pltpu.VMEM((count, 6 * SLOTS, line), jnp.bfloat16),
            pltpu.VMEM((count, SLOTS, line), jnp.float32),
            pltpu.VMEM((count, SLOTS, line), jnp.float32),
            pltpu.VMEM((4, MARINE_STRATA, line), jnp.float32),
            pltpu.VMEM((4, MARINE_STRATA, line), jnp.float32),
            pltpu.VMEM((MARINE_STRATA, OX + 16, line), jnp.float32),
            pltpu.VMEM((2 + MARINE_STRATA, OX, line), jnp.float32),
            pltpu.VMEM((7, 2, WIDE, line), jnp.float32),
        ]
        + boxes(4)
        + boxes(3)
        + boxes(3)
        + [pltpu.SemaphoreType.DMA]
        + [pltpu.SemaphoreType.DMA((count,))] * 4
        + [pltpu.SemaphoreType.DMA((4,))] * 2
        + [pltpu.SemaphoreType.DMA((10,))] * 6,
        compiler_params=pltpu.CompilerParams(collective_id=0, has_side_effects=True),
        name="window",
    )(
        sky_interface_transfers,
        coupling_matrix_enlarged,
        piece_keeper_part.reshape(1, NB),
        receiving_part_line,
        marine_point_switch,
        potential_heat_deviation,
        free_marine_lift,
        depth_averaged_uflow,
        depth_averaged_vflow,
    )
    anywhere = pl.BlockSpec(memory_space=pl.ANY)
    return pl.pallas_call(
        hand_over,
        out_shape=shapes,
        in_specs=[anywhere] * 3,
        out_specs=(anywhere,) * 3,
        scratch_shapes=[pltpu.VMEM(shape.shape, jnp.float32) for shape in shapes]
        + [pltpu.SemaphoreType.DMA((3,))] * 2,
        name="hand_over",
    )(*results)


def solution(mesh):
    in_specs = (
        P(None, "gy", "gx"),
        P("gy", "gx", None),
        P("gx", "gy", None),
        P("gx", "gy"),
        P("gx", "gy"),
        P(None, "gx", "gy"),
        P("gx", "gy"),
        P("gx", "gy"),
        P("gx", "gy"),
    )
    out_specs = (P("gy", "gx"), P(None, "gx", "gy"), P(None, "gx", "gy"))
    return jax.shard_map(
        per_device, mesh=mesh, in_specs=in_specs, out_specs=out_specs, check_vma=False
    )
```
